1024 devices in a mesh: ctx: 64 (over y, x), tp: 8 (over z), grp: 2 (over core).
Axes of the slice: x: 8, y: 8, z: 8, core: 2. Of those that a mesh axis runs over, the one named last changes fastest.
Arguments:
- patches: bfloat16 [8192, 5120], P('ctx'), may hold values from -6 to 6
- route_count: int32 [64, 64], replicated, may hold values from 0 to 2, as said below
- text_states: bfloat16 [8192, 4096], P('ctx', ('tp', 'grp')), may hold values from -6 to 6
- segment_ids: int32 [8192], replicated, may hold values from 0 to 3, never falling along the last dimension, each value on 1 to 4096 neighbouring positions
- vision_gain: float32 [1280], replicated, may hold values from 0.1 to 1.9
- merge_up: bfloat16 [5120, 2560], P(None, ('tp', 'grp')), may hold values from -0.078125 to 0.078125
- merge_down: bfloat16 [2560, 4096], P(('tp', 'grp')), may hold values from -0.125 to 0.125
- norm_gain: float32 [4096], replicated, may hold values from 0.1 to 1.9
- query_weight: bfloat16 [4096, 4096], P(None, ('tp', 'grp')), may hold values from -0.62928387 to 0.62928387
- kv_weight: bfloat16 [4096, 2048], P(None, 'tp'), may hold values from -0.4578688 to 0.4578688
Outputs:
- attended: bfloat16 [8192, 4096], P('ctx', ('tp', 'grp'))
The draws below stay inside these ranges and needn't reach their ends.
Inputs may be any that keep to these rules, and one draw needn't show every extreme that they name: route_count[c, d] counts the live rows among the 2 rows that source c holds for owner d; at least one owner gets 2 live rows from every source. `segment_ids`: never falling along the packed batch; a segment has at most 4096 positions.
All inputs are finite; a program needn't handle non-finite values.
Results may differ from the reference program's by a relative error of at most 0.04.
Values may be sent and summed in bfloat16 or wider, within the bound.
No kernel may reach another device: no remote copies, remote signals or barrier semaphores. Data moves between devices by JAX's collectives and lax.ppermute only.
A program may use at most 64 MiB of HBM per device.

```python
import math
import jax
import jax.numpy as jnp
import numpy as np
from jax import lax

VIS = 1280
DIN = 5120
F = 2560
D = 4096
HQ = 32
KVH = 8
HD = 128
CAP = 2
TOK_DEV = 128
TOKENS = 8192
PATCH_ROWS = 8192
N_CTX = 64


def draw_route_count(key, part):
    counts_low = jax.random.randint(jax.random.fold_in(key, 11), (N_CTX, N_CTX), 0, CAP + 1)
    full_owner = jax.random.randint(jax.random.fold_in(key, 12), (), 0, N_CTX)
    full_column = jnp.arange(N_CTX)[None, :] == full_owner
    return jnp.where(full_column, CAP, counts_low).astype(jnp.int32)


def draw_query_weight(key, part):
    base = jnp.clip(jax.random.normal(jax.random.fold_in(key, 911), (D, HQ * HD), jnp.float32), -6.0, 6.0) * (8.0 / D) ** 0.5
    return base.astype(jnp.bfloat16)


def draw_kv_weight(key, part):
    base = jnp.clip(jax.random.normal(jax.random.fold_in(key, 921), (D, 2 * KVH * HD), jnp.float32), -6.0, 6.0) * D ** (-0.5)
    return base.astype(jnp.bfloat16)


def block_scale(own_key, dims, shards, smallest, top_value):
    def one(axis_at, blocks):
        draws = jax.random.uniform(jax.random.fold_in(jax.random.fold_in(own_key, 6), axis_at), (blocks,), jnp.float32, smallest / len(shards), top_value / len(shards))
        return jnp.repeat(jnp.exp(draws), dims[axis_at] // blocks).reshape((-1,) + (1,) * (len(dims) - axis_at - 1))

    loudness = one(*shards[0])
    for cut in shards[1:]:
        loudness = loudness * one(*cut)
    return loudness


def split_up(amount, total, reach, skew):
    loads = [(1 << 20) // math.isqrt(rank ** skew) + 1 for rank in range(2, amount + 1)]
    rest, counts = total - reach - (amount - 1), [1] * (amount - 1)
    while rest > 0:
        free = [i for i in range(amount - 1) if counts[i] < reach]
        whole, remaining = sum([loads[i] for i in free]), rest
        for i in free:
            extra = min(reach - counts[i], max(1, remaining * loads[i] // whole), rest)
            counts[i] = counts[i] + extra
            rest = rest - extra
    return np.array([reach] + counts)


def ragged(stream_key, count, total, most, slope):
    if count == 2:
        one = jax.random.randint(stream_key, (), max(1, total - most), min(most, total - 1) + 1)
        return jnp.stack([one, total - one])
    sizes = jnp.asarray(split_up(count, total, most, slope), jnp.int32)
    pairs = (count - 1) // 2
    source_of, receiver = sizes[1:1 + 2 * pairs:2], sizes[2:2 + 2 * pairs:2]
    room = jnp.minimum(source_of - 1, most - receiver)
    passed = jax.random.randint(jax.random.fold_in(stream_key, 1), (pairs,), 0, 1 << 20) % (room + 1)
    sizes = sizes.at[1:1 + 2 * pairs:2].set(source_of - passed).at[2:2 + 2 * pairs:2].set(receiver + passed)
    return sizes[jax.random.permutation(jax.random.fold_in(stream_key, 2), count)]


def noise(own_key, shape, scale, limit, shards=(), held_as=jnp.bfloat16):
    drawn = scale * jax.random.normal(own_key, shape, jnp.float32)
    if shards:
        drawn = drawn * block_scale(own_key, shape, shards, -0.22, 0.18)
    return jnp.clip(drawn, -limit, limit).astype(held_as)


def setup_inputs(seed: int = 0) -> dict:
    seeds = jax.random.split(jax.random.key(seed), 11)
    return {
        "patches": noise(seeds[0], (PATCH_ROWS, DIN), 1.0, 6.0, ((0, 64),)),
        "route_count": draw_route_count(jax.random.fold_in(seeds[10], 71), 0),
        "text_states": noise(seeds[2], (TOKENS, D), 1.0, 6.0, ((0, 64), (1, 16))),
        "segment_ids": jnp.searchsorted(jnp.cumsum(ragged(seeds[3], 4, TOKENS, TOKENS // 2, 0)), jnp.arange(TOKENS), side="right").astype(jnp.int32),
        "vision_gain": jnp.clip(1.0 + 0.18 * jax.random.normal(seeds[4], (VIS,), jnp.float32), 0.1, 1.9),
        "merge_up": noise(seeds[5], (DIN, F), DIN ** -0.5, 0.078125, ((1, 16),)),
        "merge_down": noise(seeds[6], (F, D), F ** -0.5, 0.125, ((0, 16),)),
        "norm_gain": jnp.clip(1.0 + 0.18 * jax.random.normal(seeds[7], (D,), jnp.float32), 0.1, 1.9),
        "query_weight": draw_query_weight(jax.random.fold_in(seeds[10], 71), 0),
        "kv_weight": draw_kv_weight(jax.random.fold_in(seeds[10], 71), 0),
    }


EPSILON = 1e-06
NEGATIVE = -1e+30

def reference(patches, route_count, text_states, segment_ids, vision_gain, merge_up, merge_down, norm_gain, query_weight, kv_weight):
    grouped = patches.astype(jnp.float32).reshape(PATCH_ROWS, 4, VIS)
    mean_square = lax.optimization_barrier(jnp.mean(grouped * grouped, axis=-1, keepdims=True))
    patch_normed = (grouped * lax.rsqrt(mean_square + EPSILON) * vision_gain).reshape(PATCH_ROWS, DIN).astype(jnp.bfloat16)
    hidden = jax.nn.gelu(jnp.dot(patch_normed, merge_up, preferred_element_type=jnp.float32), approximate=False).astype(jnp.bfloat16)
    merged = jnp.dot(hidden, merge_down, preferred_element_type=jnp.float32).astype(jnp.bfloat16)
    by_owner = merged.reshape(N_CTX, N_CTX, CAP, D).transpose(1, 0, 2, 3).reshape(N_CTX, N_CTX * CAP, D)
    count_ends = jnp.cumsum(route_count, axis=0).astype(jnp.int32)
    count_starts = (count_ends - route_count).astype(jnp.int32)
    slot_ids = jnp.arange(TOK_DEV, dtype=jnp.int32)
    source = lax.optimization_barrier(jnp.sum((count_ends.T[:, None, :] <= slot_ids[None, :, None]).astype(jnp.int32), axis=2)).astype(jnp.int32)
    source = jnp.minimum(source, N_CTX - 1)
    source_match = source[:, :, None] == jnp.arange(N_CTX, dtype=jnp.int32)[None, None, :]
    first_slot = lax.optimization_barrier(jnp.sum(jnp.where(source_match, count_starts.T[:, None, :], 0), axis=2)).astype(jnp.int32)
    visual = slot_ids[None, :] < count_ends[N_CTX - 1][:, None]
    pick_rows = jnp.where(visual, source * CAP + slot_ids[None, :] - first_slot, 0).astype(jnp.int32)
    visual_rows = jnp.take_along_axis(by_owner, pick_rows[:, :, None], axis=1)
    packed = jnp.where(visual[:, :, None], visual_rows, text_states.reshape(N_CTX, TOK_DEV, D)).reshape(TOKENS, D)
    packed_f = packed.astype(jnp.float32)
    mean_packed = lax.optimization_barrier(jnp.mean(packed_f * packed_f, axis=-1, keepdims=True))
    normal = (packed_f * lax.rsqrt(mean_packed + EPSILON) * norm_gain).astype(jnp.bfloat16)
    queries = jnp.dot(normal, query_weight, preferred_element_type=jnp.float32).astype(jnp.bfloat16).reshape(TOKENS, HQ, HD)
    kv_pairs = jnp.dot(normal, kv_weight, preferred_element_type=jnp.float32).astype(jnp.bfloat16).reshape(TOKENS, KVH, 2, HD)
    positions = jnp.arange(TOKENS, dtype=jnp.int32)
    visual_count = lax.optimization_barrier(jnp.sum(route_count, axis=0)).astype(jnp.int32)
    key_visual = positions % TOK_DEV < jnp.repeat(visual_count, TOK_DEV)
    allowed = (segment_ids[:, None] == segment_ids[None, :]) & (key_visual[None, :] | (positions[None, :] <= positions[:, None]))
    group = HQ // KVH

    def one_head(head_index):
        query_head = lax.dynamic_index_in_dim(queries, head_index, 1, keepdims=False)
        kv_pair = lax.dynamic_index_in_dim(kv_pairs, head_index // group, 1, keepdims=False)
        key_head = kv_pair[:, 0]
        value_head = kv_pair[:, 1]
        scores = jnp.dot(query_head, key_head.T, preferred_element_type=jnp.float32) * HD ** (-0.5)
        masked = jnp.where(allowed, scores, NEGATIVE)
        row_max = lax.optimization_barrier(jnp.max(masked, axis=1, keepdims=True))
        weights = jnp.where(allowed, jnp.exp(masked - row_max), 0.0)
        denominator = lax.optimization_barrier(jnp.sum(weights, axis=1, keepdims=True))
        mixed = jnp.dot(weights.astype(jnp.bfloat16), value_head, preferred_element_type=jnp.float32)
        return (mixed / denominator).astype(jnp.bfloat16)
    heads = lax.map(one_head, jnp.arange(HQ, dtype=jnp.int32))
    return heads.transpose(1, 0, 2).reshape(TOKENS, HQ * HD)
```

```python
import functools

import jax
import jax.numpy as jnp
from jax import lax
from jax.experimental import pallas as pl
from jax.experimental.pallas import tpu as pltpu
from jax.sharding import Mesh
from jax.sharding import PartitionSpec as P

HD = 128
EPSILON = 1e-06
NEGATIVE = -1e30
LOG2E = 1.4426950408889634
F32 = jnp.float32
BF16 = jnp.bfloat16
VMEM = pl.BlockSpec(memory_space=pltpu.VMEM)
SMEM = pl.BlockSpec(memory_space=pltpu.SMEM)


def params(*semantics):
    return pltpu.CompilerParams(
        dimension_semantics=semantics or None, vmem_limit_bytes=40 << 20
    )


def exchange(parts, axis, dim=0):
    return lax.all_to_all(parts, axis, split_axis=dim, concat_axis=dim, tiled=True)


def up_kernel(x_ref, gain_ref, w_ref, out_ref, acc_ref):
    step = pl.program_id(0)
    x = x_ref[...].astype(F32)
    scale = lax.rsqrt(jnp.mean(x * x, axis=-1, keepdims=True) + EPSILON)
    normed = (x * scale * gain_ref[...]).astype(BF16)
    product = jnp.dot(normed, w_ref[...], preferred_element_type=F32)

    @pl.when(step == 0)
    def _():
        acc_ref[...] = product

    @pl.when(step > 0)
    def _():
        acc_ref[...] += product

    @pl.when(step == pl.num_programs(0) - 1)
    def _():
        total = acc_ref[...]
        out_ref[...] = (0.5 * total * (1.0 + lax.erf(total * 0.5**0.5))).astype(BF16)


def merge_up_rows(patches, vision_gain, merge_up):
    rows, width = patches.shape
    vis = vision_gain.shape[0]
    units = merge_up.shape[1]
    return pl.pallas_call(
        up_kernel,
        grid=(width // vis,),
        in_specs=[
            pl.BlockSpec((rows, vis), lambda k: (0, k)),
            pl.BlockSpec((1, vis), lambda k: (0, 0)),
            pl.BlockSpec((vis, units), lambda k: (k, 0)),
        ],
        out_specs=pl.BlockSpec((rows, units), lambda k: (0, 0)),
        out_shape=jax.ShapeDtypeStruct((rows, units), BF16),
        scratch_shapes=[pltpu.VMEM((rows, units), F32)],
        compiler_params=params("arbitrary"),
        name="merge_up",
    )(patches, vision_gain.reshape(1, vis), merge_up)


def owner_column(owner, route):
    lanes = lax.broadcasted_iota(jnp.int32, route.shape, 1)
    return jnp.sum(jnp.where(lanes == owner, route, 0), axis=1, keepdims=True)


def down_kernel(owner_ref, route_ref, arrived_ref, w_ref, out_ref, pick_ref):
    step = pl.program_id(0)

    @pl.when(step == 0)
    def _():
        rows = arrived_ref.shape[0]
        sources = route_ref.shape[0]
        bucket = rows // sources
        column = owner_column(owner_ref[0], route_ref[...])
        source = lax.broadcasted_iota(jnp.int32, (sources, rows), 0)
        row = lax.broadcasted_iota(jnp.int32, (sources, rows), 1)
        before = jnp.sum(
            jnp.where(source * bucket + bucket <= row, column, 0), axis=0, keepdims=True
        )
        own = (source * bucket <= row) & (row < source * bucket + bucket)
        count = jnp.sum(jnp.where(own, column, 0), axis=0, keepdims=True)
        place = lax.rem(lax.broadcasted_iota(jnp.int32, (1, rows), 1), bucket)
        target = jnp.where(place < count, before + place, -1)
        slot = lax.broadcasted_iota(jnp.int32, (rows, rows), 0)
        select = jnp.where(slot == target, 1.0, 0.0).astype(BF16)
        pick_ref[...] = jnp.dot(
            select, arrived_ref[...], preferred_element_type=F32
        ).astype(BF16)

    out_ref[0, 0] = jnp.dot(
        pick_ref[...], w_ref[...], preferred_element_type=F32
    ).astype(BF16)


def merge_down_rows(owner, route_count, arrived, merge_down, tp, grp):
    rows, units = arrived.shape
    width = merge_down.shape[1] // (tp * grp)
    return pl.pallas_call(
        down_kernel,
        grid=(tp * grp,),
        in_specs=[
            SMEM,
            VMEM,
            VMEM,
            pl.BlockSpec((units, width), lambda k: (0, k)),
        ],
        out_specs=pl.BlockSpec((1, 1, rows, width), lambda k: (k % grp, k // grp, 0, 0)),
        out_shape=jax.ShapeDtypeStruct((grp, tp, rows, width), BF16),
        scratch_shapes=[pltpu.VMEM((rows, units), BF16)],
        compiler_params=params("arbitrary"),
        name="merge_down",
    )(owner, route_count, arrived, merge_down)


def pair_kernel(parts_ref, out_ref):
    out_ref[...] = (parts_ref[0].astype(F32) + parts_ref[1].astype(F32)).astype(BF16)


def pair_sum(parts):
    return pl.pallas_call(
        pair_kernel,
        in_specs=[VMEM],
        out_specs=VMEM,
        out_shape=jax.ShapeDtypeStruct(parts.shape[1:], BF16),
        compiler_params=params(),
        name="pair_sum",
    )(parts)


def place_kernel(owner_ref, route_ref, parts_ref, text_ref, out_ref):
    total = parts_ref[0].astype(F32)
    for k in range(1, parts_ref.shape[0]):
        total += parts_ref[k].astype(F32)
    visual = jnp.sum(owner_column(owner_ref[0], route_ref[...]), axis=0, keepdims=True)
    slot = lax.broadcasted_iota(jnp.int32, total.shape, 0)
    placed = jnp.where(slot < visual, total, text_ref[...].astype(F32)).astype(BF16)
    for k in range(out_ref.shape[0]):
        out_ref[k] = placed


def place_rows(owner, route_count, parts, text_states):
    return pl.pallas_call(
        place_kernel,
        in_specs=[SMEM, VMEM, VMEM, VMEM],
        out_specs=VMEM,
        out_shape=jax.ShapeDtypeStruct(parts.shape, BF16),
        compiler_params=params(),
        name="place",
    )(owner, route_count, parts, text_states)


def project_kernel(parts_ref, gain_ref, wq_ref, wkv_ref, q_ref, kv_ref):
    grp, tp, rows, width = parts_ref.shape
    squares = jnp.zeros((rows, width), F32)
    for g in range(grp):
        for t in range(tp):
            x = parts_ref[g, t].astype(F32)
            squares += x * x
    mean = jnp.sum(squares, axis=-1, keepdims=True) / (grp * tp * width)
    scale = lax.rsqrt(mean + EPSILON)
    q = jnp.zeros((rows, wq_ref.shape[1]), F32)
    kv = jnp.zeros((rows, wkv_ref.shape[1]), F32)
    for t in range(tp):
        for g in range(grp):
            lo = (t * grp + g) * width
            gain = gain_ref[:, lo : lo + width]
            normal = (parts_ref[g, t].astype(F32) * scale * gain).astype(BF16)
            q += jnp.dot(normal, wq_ref[lo : lo + width, :], preferred_element_type=F32)
            kv += jnp.dot(normal, wkv_ref[lo : lo + width, :], preferred_element_type=F32)
    q = q.astype(BF16)
    kv = kv.astype(BF16)
    for k in range(q_ref.shape[0]):
        q_ref[k] = q
    for k in range(kv_ref.shape[0]):
        kv_ref[k] = kv


def project(parts, norm_gain, query_weight, kv_weight, q_copies, kv_copies):
    rows = parts.shape[2]
    return pl.pallas_call(
        project_kernel,
        in_specs=[VMEM] * 4,
        out_specs=[VMEM] * 2,
        out_shape=[
            jax.ShapeDtypeStruct((q_copies, rows, query_weight.shape[1]), BF16),
            jax.ShapeDtypeStruct((kv_copies, rows, kv_weight.shape[1]), BF16),
        ],
        compiler_params=params(),
        name="project",
    )(parts, norm_gain.reshape(1, -1), query_weight, kv_weight)


def attend_kernel(home_ref, visual_ref, q_ref, kv_ref, seg_ref, out_ref):
    _, rows, q_width = q_ref.shape
    q_blocks = pl.num_programs(0)
    kv_blocks = kv_ref.shape[0]
    heads = q_width // HD
    row_home = home_ref[0]
    column_home = home_ref[1]
    block = pl.program_id(0)
    q_block = row_home * q_blocks + block
    lanes = lax.broadcasted_iota(jnp.int32, (rows, rows), 1)
    q_seg = jnp.broadcast_to(seg_ref[pl.ds(q_block, 1), :], (rows, rows)).T
    q_pos = q_block * rows + lax.broadcasted_iota(jnp.int32, (rows, rows), 0)
    q = jnp.concatenate([q_ref[0, :, h * HD : (h + 1) * HD] for h in range(heads)], axis=0)
    scores = []
    top = None
    for k in range(kv_blocks):
        k_block = k * q_blocks + column_home
        seen_from = jnp.where(lanes < visual_ref[k_block], -1, k_block * rows + lanes)
        k_seg = seg_ref[pl.ds(k_block, 1), :]
        allowed = (q_seg == k_seg) & (seen_from <= q_pos)
        s = lax.dot_general(
            q, kv_ref[k, :, :HD], (((1,), (1,)), ((), ())), preferred_element_type=F32
        ) * (HD**-0.5 * LOG2E)
        s = jnp.concatenate(
            [jnp.where(allowed, s[h * rows : (h + 1) * rows], NEGATIVE) for h in range(heads)],
            axis=0,
        )
        scores.append(s)
        top = s if top is None else jnp.maximum(top, s)
    top = jnp.max(top, axis=1, keepdims=True)
    floor = jnp.maximum(top, 0.5 * NEGATIVE)
    total = jnp.zeros((heads * rows, rows), F32)
    mixed = jnp.zeros((heads * rows, HD), F32)
    for k in range(kv_blocks):
        weights = jnp.exp2(scores[k] - floor)
        total += weights
        mixed += jnp.dot(
            weights.astype(BF16), kv_ref[k, :, HD:], preferred_element_type=F32
        )
    total = jnp.sum(total, axis=1, keepdims=True)
    empty = total == 0.0
    mixed = mixed / jnp.where(empty, 1.0, total)
    mass = jnp.where(empty, NEGATIVE, floor + jnp.log2(jnp.where(empty, 1.0, total)))
    for h in range(heads):
        cols = slice(h * HD, (h + 1) * HD)
        part = slice(h * rows, (h + 1) * rows)
        out_ref[0, :rows, cols] = mixed[part].astype(BF16)
        flat = jnp.broadcast_to(mass[part], (rows, rows)).T[:16]
        high = flat.astype(BF16).astype(F32)
        low = flat - high
        second = lax.broadcasted_iota(jnp.int32, flat.shape, 0) >= 8
        out_ref[0, rows:, cols] = jnp.where(second, low, high).astype(BF16)


def attend(home, visual_count, q_parts, kv_parts, segment_rows):
    q_blocks, rows, width = q_parts.shape
    return pl.pallas_call(
        attend_kernel,
        grid=(q_blocks,),
        in_specs=[
            SMEM,
            SMEM,
            pl.BlockSpec((1, rows, width), lambda k: (k, 0, 0)),
            VMEM,
            VMEM,
        ],
        out_specs=pl.BlockSpec((1, rows + 16, width), lambda k: (k, 0, 0)),
        out_shape=jax.ShapeDtypeStruct((q_blocks, rows + 16, width), BF16),
        compiler_params=params("arbitrary"),
        name="attend",
    )(home, visual_count, q_parts, kv_parts, segment_rows)


def combine_kernel(parts_ref, out_ref):
    count = parts_ref.shape[0]
    rows, width = out_ref.shape
    for h in range(width // HD):
        cols = slice(h * HD, (h + 1) * HD)
        masses = []
        for k in range(count):
            stats = parts_ref[k, rows:, cols].astype(F32)
            flat = stats[0:1] + stats[8:9]
            masses.append(jnp.broadcast_to(flat, (rows, HD)).T)
        top = functools.reduce(jnp.maximum, masses)
        total = jnp.zeros((rows, HD), F32)
        mixed = jnp.zeros((rows, HD), F32)
        for k in range(count):
            weight = jnp.exp2(masses[k] - top)
            total += weight
            mixed += weight * parts_ref[k, :rows, cols].astype(F32)
        out_ref[:, cols] = (mixed / total).astype(BF16)


def combine(parts):
    return pl.pallas_call(
        combine_kernel,
        in_specs=[VMEM],
        out_specs=VMEM,
        out_shape=jax.ShapeDtypeStruct((parts.shape[1] - 16, parts.shape[2]), BF16),
        compiler_params=params(),
        name="combine",
    )(parts)


def shards(
    patches,
    route_count,
    text_states,
    segment_ids,
    vision_gain,
    merge_up,
    merge_down,
    norm_gain,
    query_weight,
    kv_weight,
):
    tp, grp = lax.axis_size("tp"), lax.axis_size("grp")
    n_y, n_x = lax.axis_size("ctx_0"), lax.axis_size("ctx_1")
    y, x = lax.axis_index("ctx_0"), lax.axis_index("ctx_1")
    rows = patches.shape[0]
    home = jnp.stack([y, x]).astype(jnp.int32)
    owner = (y * n_x + x).astype(jnp.int32).reshape(1)
    visual_count = jnp.sum(route_count, axis=0)
    segment_rows = segment_ids.reshape(-1, rows)

    hidden = merge_up_rows(patches, vision_gain, merge_up)
    units = hidden.shape[1]
    hidden = hidden.reshape(n_y, n_x, rows // (n_y * n_x), units)
    hidden = exchange(hidden, "ctx_0", 0)
    hidden = exchange(hidden, "ctx_1", 1)
    partial_sums = merge_down_rows(
        owner, route_count, hidden.reshape(rows, units), merge_down, tp, grp
    )
    partial_sums = pair_sum(exchange(partial_sums, "grp"))
    partial_sums = exchange(partial_sums, "tp")
    placed = place_rows(owner, route_count, partial_sums, text_states)
    packed = exchange(placed, "tp")
    packed = exchange(jnp.broadcast_to(packed[None], (grp, *packed.shape)), "grp")
    packed = packed.reshape(grp, tp, rows, -1)
    q, kv = project(packed, norm_gain, query_weight, kv_weight, n_x, n_y)
    kv = exchange(kv, "ctx_0")
    q = exchange(q, "ctx_1")
    parts = attend(home, visual_count, q, kv, segment_rows)
    return combine(exchange(parts, "ctx_1"))


def solution(mesh):
    finer = Mesh(
        mesh.devices.reshape(8, 8, mesh.shape["tp"], mesh.shape["grp"]),
        ("ctx_0", "ctx_1", "tp", "grp"),
    )
    ctx = ("ctx_0", "ctx_1")
    return jax.shard_map(
        shards,
        mesh=finer,
        in_specs=(
            P(ctx, None),
            P(),
            P(ctx, ("tp", "grp")),
            P(),
            P(),
            P(None, ("tp", "grp")),
            P(("tp", "grp"), None),
            P(),
            P(None, ("tp", "grp")),
            P(None, "tp"),
        ),
        out_specs=P(ctx, ("tp", "grp")),
        check_vma=False,
    )
```

```python
import functools

import jax
import jax.numpy as jnp
from jax import lax
from jax.experimental import pallas as pl
from jax.experimental.pallas import tpu as pltpu
from jax.sharding import Mesh
from jax.sharding import PartitionSpec as P

HD = 128
CTX = ("ctx_0", "ctx_q", "ctx_p")
EPSILON = 1e-06
NEGATIVE = -1e30
LOG2E = 1.4426950408889634
F32 = jnp.float32
BF16 = jnp.bfloat16
VMEM = pl.BlockSpec(memory_space=pltpu.VMEM)
SMEM = pl.BlockSpec(memory_space=pltpu.SMEM)


def params(*semantics):
    return pltpu.CompilerParams(
        dimension_semantics=semantics or None, vmem_limit_bytes=40 << 20
    )


def exchange(parts, axis):
    return lax.all_to_all(parts, axis, split_axis=0, concat_axis=0, tiled=True)


def up_kernel(x_hbm, gain_hbm, w_hbm, out_ref, x_ref, gain_ref, w_ref, sems, gain_sem):
    groups, rows, vis = x_ref.shape
    gain_copy = pltpu.make_async_copy(gain_hbm, gain_ref, gain_sem)
    gain_copy.start()
    copies = []
    for k in range(groups):
        cols = pl.ds(k * vis, vis)
        both = (
            pltpu.make_async_copy(x_hbm.at[:, cols], x_ref.at[k], sems.at[0, k]),
            pltpu.make_async_copy(w_hbm.at[:, cols], w_ref.at[k], sems.at[1, k]),
        )
        for copy in both:
            copy.start()
        copies.append(both)
    gain_copy.wait()
    gain = gain_ref[...].reshape(1, vis)
    total = jnp.zeros((rows, w_ref.shape[1]), F32)
    for k in range(groups):
        for copy in copies[k]:
            copy.wait()
        x = x_ref[k].astype(F32)
        scale = lax.rsqrt(jnp.mean(x * x, axis=-1, keepdims=True) + EPSILON)
        normed = (x * scale * gain).astype(BF16)
        total += lax.dot_general(
            normed, w_ref[k], (((1,), (1,)), ((), ())), preferred_element_type=F32
        )
    hidden = 0.5 * total * (1.0 + lax.erf(total * 0.5**0.5))
    out_ref[...] = hidden.astype(BF16).reshape(out_ref.shape)


def merge_up_rows(patches, vision_gain, merge_up, blocks):
    rows, width = patches.shape
    vis = vision_gain.shape[0]
    units = merge_up.shape[1]
    groups = width // vis
    return pl.pallas_call(
        up_kernel,
        in_specs=[pl.BlockSpec(memory_space=pltpu.HBM)] * 3,
        out_specs=VMEM,
        out_shape=jax.ShapeDtypeStruct((blocks, rows // blocks, units), BF16),
        scratch_shapes=[
            pltpu.VMEM((groups, rows, vis), BF16),
            pltpu.VMEM((vis,), F32),
            pltpu.VMEM((groups, units, vis), BF16),
            pltpu.SemaphoreType.DMA((2, groups)),
            pltpu.SemaphoreType.DMA,
        ],
        compiler_params=params(),
        name="merge_up",
    )(patches, vision_gain, merge_up.T)


def shuffle_kernel(n_x, rows_ref, out_ref):
    n_y, inner, units = rows_ref.shape
    total, bucket = n_y * inner, inner // n_x
    target = lax.broadcasted_iota(jnp.int32, (total, total), 0)
    row = lax.broadcasted_iota(jnp.int32, (total, total), 1)
    to_x, rest = target // (n_y * bucket), target % (n_y * bucket)
    wanted = (rest // bucket) * inner + to_x * bucket + rest % bucket
    select = jnp.where(row == wanted, 1.0, 0.0).astype(BF16)
    rows = rows_ref[...].reshape(total, units)
    out = jnp.dot(select, rows, preferred_element_type=F32).astype(BF16)
    out_ref[...] = out.reshape(out_ref.shape)


def shuffle_rows(rows, n_x):
    n_y, inner, units = rows.shape
    return pl.pallas_call(
        functools.partial(shuffle_kernel, n_x),
        in_specs=[VMEM],
        out_specs=VMEM,
        out_shape=jax.ShapeDtypeStruct((n_x, n_y * inner // n_x, units), BF16),
        compiler_params=params(),
        name="shuffle",
    )(rows)


def owner_column(owner, route):
    lanes = lax.broadcasted_iota(jnp.int32, route.shape, 1)
    return jnp.sum(jnp.where(lanes == owner, route, 0), axis=1, keepdims=True)


def down_kernel(n_y, n_x, owner_ref, route_ref, arrived_ref, w_ref, out_ref):
    grp, tp, rows, width = out_ref.shape
    sources = route_ref.shape[0]
    bucket = rows // sources
    column = owner_column(owner_ref[0], route_ref[...])
    source = lax.broadcasted_iota(jnp.int32, (sources, rows), 0)
    row = lax.broadcasted_iota(jnp.int32, (sources, rows), 1)
    sender = (row // bucket % n_y) * n_x + row // (bucket * n_y)
    before = jnp.sum(jnp.where(source < sender, column, 0), axis=0, keepdims=True)
    count = jnp.sum(jnp.where(source == sender, column, 0), axis=0, keepdims=True)
    place = lax.rem(lax.broadcasted_iota(jnp.int32, (1, rows), 1), bucket)
    target = jnp.where(place < count, before + place, -1)
    slot = lax.broadcasted_iota(jnp.int32, (rows, rows), 0)
    select = jnp.where(slot == target, 1.0, 0.0).astype(BF16)
    picked = jnp.dot(select, arrived_ref[...], preferred_element_type=F32).astype(BF16)
    for t in range(tp):
        for g in range(grp):
            lo = (t * grp + g) * width
            out_ref[g, t] = jnp.dot(
                picked, w_ref[:, lo : lo + width], preferred_element_type=F32
            ).astype(BF16)


def merge_down_rows(owner, route_count, arrived, merge_down, n_y, n_x, tp, grp):
    width = merge_down.shape[1] // (tp * grp)
    return pl.pallas_call(
        functools.partial(down_kernel, n_y, n_x),
        in_specs=[SMEM, VMEM, VMEM, VMEM],
        out_specs=VMEM,
        out_shape=jax.ShapeDtypeStruct((grp, tp, arrived.shape[0], width), BF16),
        compiler_params=params(),
        name="merge_down",
    )(owner, route_count, arrived, merge_down)


def pair_kernel(parts_ref, out_ref):
    out_ref[...] = (parts_ref[0].astype(F32) + parts_ref[1].astype(F32)).astype(BF16)


def pair_sum(parts):
    return pl.pallas_call(
        pair_kernel,
        in_specs=[VMEM],
        out_specs=VMEM,
        out_shape=jax.ShapeDtypeStruct(parts.shape[1:], BF16),
        compiler_params=params(),
        name="pair_sum",
    )(parts)


def place_kernel(owner_ref, route_ref, parts_ref, text_ref, out_ref):
    total = parts_ref[0].astype(F32)
    for k in range(1, parts_ref.shape[0]):
        total += parts_ref[k].astype(F32)
    visual = jnp.sum(owner_column(owner_ref[0], route_ref[...]), axis=0, keepdims=True)
    slot = lax.broadcasted_iota(jnp.int32, total.shape, 0)
    placed = jnp.where(slot < visual, total, text_ref[...].astype(F32)).astype(BF16)
    for k in range(out_ref.shape[0]):
        out_ref[k] = placed


def place_rows(owner, route_count, parts, text_states):
    return pl.pallas_call(
        place_kernel,
        in_specs=[SMEM, VMEM, VMEM, VMEM],
        out_specs=VMEM,
        out_shape=jax.ShapeDtypeStruct(parts.shape, BF16),
        compiler_params=params(),
        name="place",
    )(owner, route_count, parts, text_states)


def project_kernel(half_ref, parts_ref, gain_ref, wq_ref, wkv_ref, q_ref, kv_ref):
    grp, tp, rows, width = parts_ref.shape
    squares = jnp.zeros((rows, width), F32)
    for g in range(grp):
        for t in range(tp):
            x = parts_ref[g, t].astype(F32)
            squares += x * x
    mean = jnp.sum(squares, axis=-1, keepdims=True) / (grp * tp * width)
    scale = lax.rsqrt(mean + EPSILON)
    q = jnp.zeros((rows, wq_ref.shape[1]), F32)
    kv = jnp.zeros((rows, wkv_ref.shape[1]), F32)
    for t in range(tp):
        for g in range(grp):
            lo = (t * grp + g) * width
            gain = gain_ref[lo : lo + width].reshape(1, width)
            normal = (parts_ref[g, t].astype(F32) * scale * gain).astype(BF16)
            q += jnp.dot(normal, wq_ref[lo : lo + width, :], preferred_element_type=F32)
            kv += jnp.dot(normal, wkv_ref[lo : lo + width, :], preferred_element_type=F32)
    q = q.astype(BF16)
    for k in range(q_ref.shape[0]):
        q_ref[k] = q
    part = kv_ref.shape[1]
    own = kv[:part]
    for g in range(1, rows // part):
        own = jnp.where(half_ref[0] == g, kv[g * part : (g + 1) * part], own)
    for k in range(kv_ref.shape[0]):
        kv_ref[k] = own.astype(BF16)


def project(half, parts, norm_gain, query_weight, kv_weight, q_copies, kv_copies):
    grp, _, rows, _ = parts.shape
    return pl.pallas_call(
        project_kernel,
        in_specs=[SMEM] + [VMEM] * 4,
        out_specs=[VMEM] * 2,
        out_shape=[
            jax.ShapeDtypeStruct((q_copies, rows, query_weight.shape[1]), BF16),
            jax.ShapeDtypeStruct((kv_copies, rows // grp, kv_weight.shape[1]), BF16),
        ],
        compiler_params=params(),
        name="project",
    )(half, parts, norm_gain, query_weight, kv_weight)


def seen_kernel(route_ref, seen_ref):
    blocks, rows = seen_ref.shape
    visual = jnp.sum(route_ref[...].T, axis=1, keepdims=True)
    block = lax.broadcasted_iota(jnp.int32, (blocks, rows), 0)
    lane = lax.broadcasted_iota(jnp.int32, (blocks, rows), 1)
    seen_ref[...] = jnp.where(lane < visual, -1, block * rows + lane)


def seen_from(route_count, rows):
    return pl.pallas_call(
        seen_kernel,
        in_specs=[VMEM],
        out_specs=VMEM,
        out_shape=jax.ShapeDtypeStruct((route_count.shape[1], rows), jnp.int32),
        compiler_params=params(),
        name="seen",
    )(route_count)


def attend_kernel(pair, home_ref, ends_ref, q_ref, kv_ref, seg_ref, seen_ref, out_ref):
    _, rows, q_width = q_ref.shape
    heads = q_width // HD
    block = pl.program_id(0)
    pairs = kv_ref.shape[1] // pair
    n_x = pl.num_programs(0) * pair
    q_block = home_ref[0] * n_x + block * pair + home_ref[2]
    column = home_ref[1] * pair
    first = jnp.minimum(
        (jnp.maximum(ends_ref[0, block] - column - (pair - 1), 0) + n_x - 1) // n_x,
        pairs - 1,
    )
    last = (ends_ref[1, block] - column + n_x) // n_x - 1
    near = min(5, pairs)

    def rows_of(index, cols):
        return jnp.concatenate(
            [kv_ref[:, index * pair + w, :, cols].reshape(rows, HD) for w in range(pair)], axis=0
        )

    def attend_to(start, count):
        q_seg = jnp.broadcast_to(seg_ref[pl.ds(q_block, 1), :], (rows, rows)).T
        q_seg = jnp.concatenate([q_seg] * pair, axis=1)
        q_pos = q_block * rows + lax.broadcasted_iota(jnp.int32, (rows, pair * rows), 0)
        q = jnp.concatenate([q_ref[0, :, h * HD : (h + 1) * HD] for h in range(heads)], axis=0)
        scores = []
        top = None
        for k in range(count):
            keys = rows_of(start + k, slice(0, HD))
            wanted = [(start + k) * n_x + column + w for w in range(pair)]
            k_seg = jnp.concatenate([seg_ref[pl.ds(w, 1), :] for w in wanted], axis=1)
            seen = jnp.concatenate([seen_ref[pl.ds(w, 1), :] for w in wanted], axis=1)
            allowed = (q_seg == k_seg) & (seen <= q_pos)
            s = lax.dot_general(
                q, keys, (((1,), (1,)), ((), ())), preferred_element_type=F32
            ) * (HD**-0.5 * LOG2E)
            s = jnp.concatenate(
                [jnp.where(allowed, s[h * rows : (h + 1) * rows], NEGATIVE) for h in range(heads)],
                axis=0,
            )
            scores.append(s)
            top = s if top is None else jnp.maximum(top, s)
        top = jnp.max(top, axis=1, keepdims=True)
        floor = jnp.maximum(top, 0.5 * NEGATIVE)
        total = jnp.zeros((heads * rows, pair * rows), F32)
        mixed = jnp.zeros((heads * rows, HD), F32)
        for k in range(count):
            weights = jnp.exp2(scores[k] - floor)
            total += weights
            values = rows_of(start + k, slice(HD, 2 * HD))
            mixed += jnp.dot(weights.astype(BF16), values, preferred_element_type=F32)
        total = jnp.sum(total, axis=1, keepdims=True)
        empty = total == 0.0
        mixed = mixed / jnp.where(empty, 1.0, total)
        mass = jnp.where(empty, NEGATIVE, floor + jnp.log2(jnp.where(empty, 1.0, total)))
        for h in range(heads):
            cols = slice(h * HD, (h + 1) * HD)
            part = slice(h * rows, (h + 1) * rows)
            out_ref[0, :rows, cols] = mixed[part].astype(BF16)
            flat = jnp.broadcast_to(mass[part], (rows, rows)).T[:16]
            high = flat.astype(BF16).astype(F32)
            second = lax.broadcasted_iota(jnp.int32, flat.shape, 0) >= 8
            out_ref[0, rows:, cols] = jnp.where(second, flat - high, high).astype(BF16)

    close = last - first < near
    if near == pairs:
        attend_to(0, pairs)
    else:
        pl.when(close)(lambda: attend_to(jnp.minimum(first, pairs - near), near))
        pl.when(jnp.logical_not(close))(lambda: attend_to(0, pairs))


def attend(pair, home, ends, q_parts, kv_parts, segment_rows, seen):
    q_blocks, rows, width = q_parts.shape
    return pl.pallas_call(
        functools.partial(attend_kernel, pair),
        grid=(q_blocks,),
        in_specs=[
            SMEM,
            SMEM,
            pl.BlockSpec((1, rows, width), lambda k: (k, 0, 0)),
            VMEM,
            VMEM,
            VMEM,
        ],
        out_specs=pl.BlockSpec((1, rows + 16, width), lambda k: (k, 0, 0)),
        out_shape=jax.ShapeDtypeStruct((q_blocks, rows + 16, width), BF16),
        compiler_params=params("arbitrary"),
        name="attend",
    )(home, ends, q_parts, kv_parts, segment_rows, seen)


def combine_kernel(parts_ref, out_ref):
    count = parts_ref.shape[0]
    rows, width = out_ref.shape
    for h in range(width // HD):
        cols = slice(h * HD, (h + 1) * HD)
        masses = []
        for k in range(count):
            stats = parts_ref[k, rows:, cols].astype(F32)
            flat = stats[0:1] + stats[8:9]
            masses.append(jnp.broadcast_to(flat, (rows, HD)).T)
        top = functools.reduce(jnp.maximum, masses)
        total = jnp.zeros((rows, HD), F32)
        mixed = jnp.zeros((rows, HD), F32)
        for k in range(count):
            weight = jnp.exp2(masses[k] - top)
            total += weight
            mixed += weight * parts_ref[k, :rows, cols].astype(F32)
        out_ref[:, cols] = (mixed / total).astype(BF16)


def combine(parts):
    return pl.pallas_call(
        combine_kernel,
        in_specs=[VMEM],
        out_specs=VMEM,
        out_shape=jax.ShapeDtypeStruct((parts.shape[1] - 16, parts.shape[2]), BF16),
        compiler_params=params(),
        name="combine",
    )(parts)


def block_ends(own_rows, segment_ids, rows):
    first, last = own_rows[:, 0], own_rows[:, -1]
    below = jnp.sum((segment_ids[None] < first[:, None]).astype(jnp.int32), axis=1)
    upto = jnp.sum((segment_ids[None] <= last[:, None]).astype(jnp.int32), axis=1)
    return jnp.stack([below // rows, (upto - 1) // rows])


def shards(
    patches,
    route_count,
    text_states,
    segment_ids,
    vision_gain,
    merge_up,
    merge_down,
    norm_gain,
    query_weight,
    kv_weight,
):
    tp, grp = lax.axis_size("tp"), lax.axis_size("grp")
    n_y, n_q, pair = lax.axis_size("ctx_0"), lax.axis_size("ctx_q"), lax.axis_size("ctx_p")
    y, q_at, p_at = lax.axis_index("ctx_0"), lax.axis_index("ctx_q"), lax.axis_index("ctx_p")
    n_x, x = n_q * pair, q_at * pair + p_at
    rows = patches.shape[0]
    home = jnp.stack([y, q_at, p_at]).astype(jnp.int32)
    half = lax.axis_index("grp").astype(jnp.int32).reshape(1)
    owner = (y * n_x + x).astype(jnp.int32).reshape(1)
    segment_rows = segment_ids.reshape(-1, rows)
    own_rows = lax.dynamic_slice(
        segment_ids.reshape(n_y, n_q, pair, rows), (y, 0, p_at, 0), (1, n_q, 1, rows)
    )
    ends = block_ends(own_rows.reshape(n_q, rows), segment_ids, rows)
    seen = seen_from(route_count, rows)

    hidden = merge_up_rows(patches, vision_gain, merge_up, n_y)
    hidden = exchange(shuffle_rows(exchange(hidden, "ctx_0"), n_x), CTX[1:])
    partial_sums = merge_down_rows(
        owner, route_count, hidden.reshape(rows, -1), merge_down, n_y, n_x, tp, grp
    )
    partial_sums = pair_sum(exchange(partial_sums, "grp"))
    partial_sums = exchange(partial_sums, "tp")
    placed = place_rows(owner, route_count, partial_sums, text_states)
    packed = exchange(placed, "tp")
    packed = exchange(jnp.broadcast_to(packed[None], (grp, *packed.shape)), "grp")
    packed = packed.reshape(grp, tp, rows, -1)
    q, kv = project(half, packed, norm_gain, query_weight, kv_weight, n_q, n_y * pair)
    kv = exchange(kv, ("ctx_0", "ctx_p"))
    kv = exchange(jnp.broadcast_to(kv[None], (grp, *kv.shape)), "grp")
    q = exchange(q, "ctx_q")
    parts = attend(pair, home, ends, q, kv, segment_rows, seen)
    return combine(exchange(parts, "ctx_q"))


def solution(mesh):
    finer = Mesh(
        mesh.devices.reshape(8, 4, 2, mesh.shape["tp"], mesh.shape["grp"]),
        (*CTX, "tp", "grp"),
    )
    ctx = CTX
    return jax.shard_map(
        shards,
        mesh=finer,
        in_specs=(
            P(ctx, None),
            P(),
            P(ctx, ("tp", "grp")),
            P(),
            P(),
            P(None, ("tp", "grp")),
            P(("tp", "grp"), None),
            P(),
            P(None, ("tp", "grp")),
            P(None, "tp"),
        ),
        out_specs=P(ctx, ("tp", "grp")),
        check_vma=False,
    )
```

```python
import functools

import jax
import jax.numpy as jnp
from jax import lax
from jax.experimental import pallas as pl
from jax.experimental.pallas import tpu as pltpu
from jax.sharding import Mesh
from jax.sharding import PartitionSpec as P

HD = 128
CTX = ("ctx_0", "ctx_q", "ctx_p")
EPSILON = 1e-06
NEGATIVE = -1e30
LOG2E = 1.4426950408889634
F32 = jnp.float32
BF16 = jnp.bfloat16
VMEM = pl.BlockSpec(memory_space=pltpu.VMEM)
SMEM = pl.BlockSpec(memory_space=pltpu.SMEM)


def params(*semantics):
    return pltpu.CompilerParams(
        dimension_semantics=semantics or None, vmem_limit_bytes=40 << 20
    )


def exchange(parts, axis):
    return lax.all_to_all(parts, axis, split_axis=0, concat_axis=0, tiled=True)


def up_kernel(x_hbm, gain_hbm, w_hbm, out_ref, x_ref, gain_ref, w_ref, sems, gain_sem):
    groups, rows, vis = x_ref.shape
    gain_copy = pltpu.make_async_copy(gain_hbm, gain_ref, gain_sem)
    gain_copy.start()
    copies = []
    for k in range(groups):
        cols = pl.ds(k * vis, vis)
        both = (
            pltpu.make_async_copy(x_hbm.at[:, cols], x_ref.at[k], sems.at[0, k]),
            pltpu.make_async_copy(w_hbm.at[:, cols], w_ref.at[k], sems.at[1, k]),
        )
        for copy in both:
            copy.start()
        copies.append(both)
    gain_copy.wait()
    gain = gain_ref[...].reshape(1, vis)
    total = jnp.zeros((rows, w_ref.shape[1]), F32)
    for k in range(groups):
        for copy in copies[k]:
            copy.wait()
        x = x_ref[k].astype(F32)
        scale = lax.rsqrt(jnp.mean(x * x, axis=-1, keepdims=True) + EPSILON)
        normed = (x * scale * gain).astype(BF16)
        total += lax.dot_general(
            normed, w_ref[k], (((1,), (1,)), ((), ())), preferred_element_type=F32
        )
    hidden = 0.5 * total * (1.0 + lax.erf(total * 0.5**0.5))
    out_ref[...] = hidden.astype(BF16).reshape(out_ref.shape)


def merge_up_rows(patches, vision_gain, merge_up, blocks):
    rows, width = patches.shape
    vis = vision_gain.shape[0]
    units = merge_up.shape[1]
    groups = width // vis
    return pl.pallas_call(
        up_kernel,
        in_specs=[pl.BlockSpec(memory_space=pltpu.HBM)] * 3,
        out_specs=VMEM,
        out_shape=jax.ShapeDtypeStruct((blocks, rows // blocks, units), BF16),
        scratch_shapes=[
            pltpu.VMEM((groups, rows, vis), BF16),
            pltpu.VMEM((vis,), F32),
            pltpu.VMEM((groups, units, vis), BF16),
            pltpu.SemaphoreType.DMA((2, groups)),
            pltpu.SemaphoreType.DMA,
        ],
        compiler_params=params(),
        name="merge_up",
    )(*[
        pltpu.with_memory_space_constraint(v, pltpu.HBM)
        for v in (patches, vision_gain, merge_up.T)
    ])


def shuffle_kernel(n_x, rows_ref, out_ref):
    n_y, inner, units = rows_ref.shape
    total, bucket = n_y * inner, inner // n_x
    target = lax.broadcasted_iota(jnp.int32, (total, total), 0)
    row = lax.broadcasted_iota(jnp.int32, (total, total), 1)
    to_x, rest = target // (n_y * bucket), target % (n_y * bucket)
    wanted = (rest // bucket) * inner + to_x * bucket + rest % bucket
    select = jnp.where(row == wanted, 1.0, 0.0).astype(BF16)
    rows = rows_ref[...].reshape(total, units)
    out = jnp.dot(select, rows, preferred_element_type=F32).astype(BF16)
    out_ref[...] = out.reshape(out_ref.shape)


def shuffle_rows(rows, n_x):
    n_y, inner, units = rows.shape
    return pl.pallas_call(
        functools.partial(shuffle_kernel, n_x),
        in_specs=[VMEM],
        out_specs=VMEM,
        out_shape=jax.ShapeDtypeStruct((n_x, n_y * inner // n_x, units), BF16),
        compiler_params=params(),
        name="shuffle",
    )(rows)


def owner_column(owner, route):
    lanes = lax.broadcasted_iota(jnp.int32, route.shape, 1)
    return jnp.sum(jnp.where(lanes == owner, route, 0), axis=1, keepdims=True)


def down_kernel(n_y, n_x, owner_ref, route_ref, arrived_ref, w_ref, out_ref):
    grp, tp, rows, width = out_ref.shape
    sources = route_ref.shape[0]
    bucket = rows // sources
    column = owner_column(owner_ref[0], route_ref[...])
    source = lax.broadcasted_iota(jnp.int32, (sources, rows), 0)
    row = lax.broadcasted_iota(jnp.int32, (sources, rows), 1)
    sender = (row // bucket % n_y) * n_x + row // (bucket * n_y)
    before = jnp.sum(jnp.where(source < sender, column, 0), axis=0, keepdims=True)
    count = jnp.sum(jnp.where(source == sender, column, 0), axis=0, keepdims=True)
    place = lax.rem(lax.broadcasted_iota(jnp.int32, (1, rows), 1), bucket)
    target = jnp.where(place < count, before + place, -1)
    slot = lax.broadcasted_iota(jnp.int32, (rows, rows), 0)
    select = jnp.where(slot == target, 1.0, 0.0).astype(BF16)
    picked = jnp.dot(select, arrived_ref[...], preferred_element_type=F32).astype(BF16)
    for t in range(tp):
        for g in range(grp):
            lo = (t * grp + g) * width
            out_ref[g, t] = jnp.dot(
                picked, w_ref[:, lo : lo + width], preferred_element_type=F32
            ).astype(BF16)


def merge_down_rows(owner, route_count, arrived, merge_down, n_y, n_x, tp, grp):
    width = merge_down.shape[1] // (tp * grp)
    return pl.pallas_call(
        functools.partial(down_kernel, n_y, n_x),
        in_specs=[SMEM, VMEM, VMEM, VMEM],
        out_specs=VMEM,
        out_shape=jax.ShapeDtypeStruct((grp, tp, arrived.shape[0], width), BF16),
        compiler_params=params(),
        name="merge_down",
    )(owner, route_count, arrived, merge_down)


def pair_kernel(parts_ref, out_ref):
    out_ref[...] = (parts_ref[0].astype(F32) + parts_ref[1].astype(F32)).astype(BF16)


def pair_sum(parts):
    return pl.pallas_call(
        pair_kernel,
        in_specs=[VMEM],
        out_specs=VMEM,
        out_shape=jax.ShapeDtypeStruct(parts.shape[1:], BF16),
        compiler_params=params(),
        name="pair_sum",
    )(parts)


def place_kernel(owner_ref, route_ref, parts_ref, text_ref, out_ref):
    total = parts_ref[0].astype(F32)
    for k in range(1, parts_ref.shape[0]):
        total += parts_ref[k].astype(F32)
    visual = jnp.sum(owner_column(owner_ref[0], route_ref[...]), axis=0, keepdims=True)
    slot = lax.broadcasted_iota(jnp.int32, total.shape, 0)
    placed = jnp.where(slot < visual, total, text_ref[...].astype(F32)).astype(BF16)
    for k in range(out_ref.shape[0]):
        out_ref[k] = placed


def place_rows(owner, route_count, parts, text_states):
    return pl.pallas_call(
        place_kernel,
        in_specs=[SMEM, VMEM, VMEM, VMEM],
        out_specs=VMEM,
        out_shape=jax.ShapeDtypeStruct(parts.shape, BF16),
        compiler_params=params(),
        name="place",
    )(owner, route_count, parts, text_states)


def project_kernel(half_ref, parts_ref, gain_ref, wq_ref, wkv_ref, q_ref, kv_ref):
    grp, tp, rows, width = parts_ref.shape
    squares = jnp.zeros((rows, width), F32)
    for g in range(grp):
        for t in range(tp):
            x = parts_ref[g, t].astype(F32)
            squares += x * x
    mean = jnp.sum(squares, axis=-1, keepdims=True) / (grp * tp * width)
    scale = lax.rsqrt(mean + EPSILON)
    q = jnp.zeros((rows, wq_ref.shape[1]), F32)
    kv = jnp.zeros((rows, wkv_ref.shape[1]), F32)
    for t in range(tp):
        for g in range(grp):
            lo = (t * grp + g) * width
            gain = gain_ref[lo : lo + width].reshape(1, width)
            normal = (parts_ref[g, t].astype(F32) * scale * gain).astype(BF16)
            q += jnp.dot(normal, wq_ref[lo : lo + width, :], preferred_element_type=F32)
            kv += jnp.dot(normal, wkv_ref[lo : lo + width, :], preferred_element_type=F32)
    q = q.astype(BF16)
    for k in range(q_ref.shape[0]):
        q_ref[k] = q
    part = kv_ref.shape[1]
    own = kv[:part]
    for g in range(1, rows // part):
        own = jnp.where(half_ref[0] == g, kv[g * part : (g + 1) * part], own)
    for k in range(kv_ref.shape[0]):
        kv_ref[k] = own.astype(BF16)


def project(half, parts, norm_gain, query_weight, kv_weight, q_copies, kv_copies):
    grp, _, rows, _ = parts.shape
    return pl.pallas_call(
        project_kernel,
        in_specs=[SMEM] + [VMEM] * 4,
        out_specs=[VMEM] * 2,
        out_shape=[
            jax.ShapeDtypeStruct((q_copies, rows, query_weight.shape[1]), BF16),
            jax.ShapeDtypeStruct((kv_copies, rows // grp, kv_weight.shape[1]), BF16),
        ],
        compiler_params=params(),
        name="project",
    )(half, parts, norm_gain, query_weight, kv_weight)


def seen_kernel(route_ref, seen_ref):
    blocks, rows = seen_ref.shape
    visual = jnp.sum(route_ref[...].T, axis=1, keepdims=True)
    block = lax.broadcasted_iota(jnp.int32, (blocks, rows), 0)
    lane = lax.broadcasted_iota(jnp.int32, (blocks, rows), 1)
    seen_ref[...] = jnp.where(lane < visual, -1, block * rows + lane)


def seen_from(route_count, rows):
    return pl.pallas_call(
        seen_kernel,
        in_specs=[VMEM],
        out_specs=VMEM,
        out_shape=jax.ShapeDtypeStruct((route_count.shape[1], rows), jnp.int32),
        compiler_params=params(),
        name="seen",
    )(route_count)


def attend_kernel(pair, home_ref, ends_ref, q_ref, kv_ref, seg_ref, seen_ref, out_ref):
    _, rows, q_width = q_ref.shape
    heads = q_width // HD
    block = pl.program_id(0)
    pairs = kv_ref.shape[1] // pair
    n_x = pl.num_programs(0) * pair
    q_block = home_ref[0] * n_x + block * pair + home_ref[2]
    column = home_ref[1] * pair
    first = jnp.minimum(
        (jnp.maximum(ends_ref[0, block] - column - (pair - 1), 0) + n_x - 1) // n_x,
        pairs - 1,
    )
    last = (ends_ref[1, block] - column + n_x) // n_x - 1
    near = min(5, pairs)

    def rows_of(index, cols):
        return jnp.concatenate(
            [kv_ref[:, index * pair + w, :, cols].reshape(rows, HD) for w in range(pair)], axis=0
        )

    def attend_to(start, count):
        q_seg = jnp.broadcast_to(seg_ref[pl.ds(q_block, 1), :], (rows, rows)).T
        q_seg = jnp.concatenate([q_seg] * pair, axis=1)
        q_pos = q_block * rows + lax.broadcasted_iota(jnp.int32, (rows, pair * rows), 0)
        q = jnp.concatenate([q_ref[0, :, h * HD : (h + 1) * HD] for h in range(heads)], axis=0)
        scores = []
        top = None
        for k in range(count):
            keys = rows_of(start + k, slice(0, HD))
            wanted = [(start + k) * n_x + column + w for w in range(pair)]
            k_seg = jnp.concatenate([seg_ref[pl.ds(w, 1), :] for w in wanted], axis=1)
            seen = jnp.concatenate([seen_ref[pl.ds(w, 1), :] for w in wanted], axis=1)
            allowed = (q_seg == k_seg) & (seen <= q_pos)
            s = lax.dot_general(
                q, keys, (((1,), (1,)), ((), ())), preferred_element_type=F32
            ) * (HD**-0.5 * LOG2E)
            s = jnp.concatenate(
                [jnp.where(allowed, s[h * rows : (h + 1) * rows], NEGATIVE) for h in range(heads)],
                axis=0,
            )
            scores.append(s)
            top = s if top is None else jnp.maximum(top, s)
        top = jnp.max(top, axis=1, keepdims=True)
        floor = jnp.maximum(top, 0.5 * NEGATIVE)
        total = jnp.zeros((heads * rows, pair * rows), F32)
        mixed = jnp.zeros((heads * rows, HD), F32)
        for k in range(count):
            weights = jnp.exp2(scores[k] - floor)
            total += weights
            values = rows_of(start + k, slice(HD, 2 * HD))
            mixed += jnp.dot(weights.astype(BF16), values, preferred_element_type=F32)
        total = jnp.sum(total, axis=1, keepdims=True)
        empty = total == 0.0
        mixed = mixed / jnp.where(empty, 1.0, total)
        mass = jnp.where(empty, NEGATIVE, floor + jnp.log2(jnp.where(empty, 1.0, total)))
        for h in range(heads):
            cols = slice(h * HD, (h + 1) * HD)
            part = slice(h * rows, (h + 1) * rows)
            out_ref[0, :rows, cols] = mixed[part].astype(BF16)
            flat = jnp.broadcast_to(mass[part], (rows, rows)).T[:16]
            high = flat.astype(BF16).astype(F32)
            second = lax.broadcasted_iota(jnp.int32, flat.shape, 0) >= 8
            out_ref[0, rows:, cols] = jnp.where(second, flat - high, high).astype(BF16)

    close = last - first < near
    if near == pairs:
        attend_to(0, pairs)
    else:
        pl.when(close)(lambda: attend_to(jnp.minimum(first, pairs - near), near))
        pl.when(jnp.logical_not(close))(lambda: attend_to(0, pairs))


def attend(pair, home, ends, q_parts, kv_parts, segment_rows, seen):
    q_blocks, rows, width = q_parts.shape
    return pl.pallas_call(
        functools.partial(attend_kernel, pair),
        grid=(q_blocks,),
        in_specs=[
            SMEM,
            SMEM,
            pl.BlockSpec((1, rows, width), lambda k: (k, 0, 0)),
            VMEM,
            VMEM,
            VMEM,
        ],
        out_specs=pl.BlockSpec((1, rows + 16, width), lambda k: (k, 0, 0)),
        out_shape=jax.ShapeDtypeStruct((q_blocks, rows + 16, width), BF16),
        compiler_params=params("arbitrary"),
        name="attend",
    )(home, ends, q_parts, kv_parts, segment_rows, seen)


def combine_kernel(parts_ref, out_ref):
    count = parts_ref.shape[0]
    rows, width = out_ref.shape
    for h in range(width // HD):
        cols = slice(h * HD, (h + 1) * HD)
        masses = []
        for k in range(count):
            stats = parts_ref[k, rows:, cols].astype(F32)
            flat = stats[0:1] + stats[8:9]
            masses.append(jnp.broadcast_to(flat, (rows, HD)).T)
        top = functools.reduce(jnp.maximum, masses)
        total = jnp.zeros((rows, HD), F32)
        mixed = jnp.zeros((rows, HD), F32)
        for k in range(count):
            weight = jnp.exp2(masses[k] - top)
            total += weight
            mixed += weight * parts_ref[k, :rows, cols].astype(F32)
        out_ref[:, cols] = (mixed / total).astype(BF16)


def combine(parts):
    return pl.pallas_call(
        combine_kernel,
        in_specs=[VMEM],
        out_specs=VMEM,
        out_shape=jax.ShapeDtypeStruct((parts.shape[1] - 16, parts.shape[2]), BF16),
        compiler_params=params(),
        name="combine",
    )(parts)


def block_ends(own_rows, segment_ids, rows):
    first, last = own_rows[:, 0], own_rows[:, -1]
    below = jnp.sum((segment_ids[None] < first[:, None]).astype(jnp.int32), axis=1)
    upto = jnp.sum((segment_ids[None] <= last[:, None]).astype(jnp.int32), axis=1)
    return jnp.stack([below // rows, (upto - 1) // rows])


def shards(
    patches,
    route_count,
    text_states,
    segment_ids,
    vision_gain,
    merge_up,
    merge_down,
    norm_gain,
    query_weight,
    kv_weight,
):
    tp, grp = lax.axis_size("tp"), lax.axis_size("grp")
    n_y, n_q, pair = lax.axis_size("ctx_0"), lax.axis_size("ctx_q"), lax.axis_size("ctx_p")
    y, q_at, p_at = lax.axis_index("ctx_0"), lax.axis_index("ctx_q"), lax.axis_index("ctx_p")
    n_x, x = n_q * pair, q_at * pair + p_at
    rows = patches.shape[0]
    home = jnp.stack([y, q_at, p_at]).astype(jnp.int32)
    half = lax.axis_index("grp").astype(jnp.int32).reshape(1)
    owner = (y * n_x + x).astype(jnp.int32).reshape(1)
    segment_rows = segment_ids.reshape(-1, rows)
    own_rows = lax.dynamic_slice(
        segment_ids.reshape(n_y, n_q, pair, rows), (y, 0, p_at, 0), (1, n_q, 1, rows)
    )
    ends = block_ends(own_rows.reshape(n_q, rows), segment_ids, rows)
    seen = seen_from(route_count, rows)

    hidden = merge_up_rows(patches, vision_gain, merge_up, n_y)
    hidden, owner, home, half = lax.optimization_barrier((hidden, owner, home, half))
    hidden = exchange(shuffle_rows(exchange(hidden, "ctx_0"), n_x), CTX[1:])
    partial_sums = merge_down_rows(
        owner, route_count, hidden.reshape(rows, -1), merge_down, n_y, n_x, tp, grp
    )
    partial_sums = pair_sum(exchange(partial_sums, "grp"))
    partial_sums = exchange(partial_sums, "tp")
    placed = place_rows(owner, route_count, partial_sums, text_states)
    packed = exchange(placed, "tp")
    packed = exchange(jnp.broadcast_to(packed[None], (grp, *packed.shape)), "grp")
    packed = packed.reshape(grp, tp, rows, -1)
    q, kv = project(half, packed, norm_gain, query_weight, kv_weight, n_q, n_y * pair)
    kv = exchange(kv, ("ctx_0", "ctx_p"))
    kv = exchange(jnp.broadcast_to(kv[None], (grp, *kv.shape)), "grp")
    q = exchange(q, "ctx_q")
    parts = attend(pair, home, ends, q, kv, segment_rows, seen)
    return combine(exchange(parts, "ctx_q"))


def solution(mesh):
    finer = Mesh(
        mesh.devices.reshape(8, 4, 2, mesh.shape["tp"], mesh.shape["grp"]),
        (*CTX, "tp", "grp"),
    )
    ctx = CTX
    return jax.shard_map(
        shards,
        mesh=finer,
        in_specs=(
            P(ctx, None),
            P(),
            P(ctx, ("tp", "grp")),
            P(),
            P(),
            P(None, ("tp", "grp")),
            P(("tp", "grp"), None),
            P(),
            P(None, ("tp", "grp")),
            P(None, "tp"),
        ),
        out_specs=P(ctx, ("tp", "grp")),
        check_vma=False,
    )
```
